32 devices in a mesh: section: 4 (over z), rep: 8 (over y, x, core).
Axes of the slice: x: 2, y: 2, z: 4, core: 2. Of those that a mesh axis runs over, the one named last changes fastest.
Arguments:
- tokens: bfloat16 [4, 1024, 1024], P(None, 'rep'), may hold values from -6 to 6
- replica_of_row: int32 [4, 1024, 1], P(None, 'rep'), may hold values from 0 to 15; in each aligned block of 128 rows (0 to 127, 128 to 255, ..., all dimensions but the last counted through in order) at most 12 rows name the same one
- widths: int32 [16], replicated, may hold values from 512 to 1024, as said below
- placement: int32 [16], replicated, may hold values from 0 to 23, as said below
- gains: float32 [4, 24, 1024], P('section', 'rep'), may hold values from 0.5 to 1.5
- weights: bfloat16 [4, 24, 1024, 1024], P('section', 'rep'), may hold values from -0.1875 to 0.1875
Outputs:
- final: bfloat16 [4, 1024, 1024], P(None, 'rep', 'section')
The draws below stay inside these ranges and needn't reach their ends.
Inputs may be any that keep to these rules, and one draw needn't show every extreme that they name: `widths`: multiples of 128 from 512 to 1024. `placement`: distinct slots; slot g lies on index g // 3 of rep. `replica_of_row`: within the 128 tokens of one index of rep in one micro-batch, no replica is named by more than 12 tokens.
All inputs are finite; a program needn't handle non-finite values.
Results may differ from the reference program's by a relative error of at most 0.008.
Values may be sent and summed in bfloat16 or wider, within the bound.
No kernel may reach another device: no remote copies, remote signals or barrier semaphores. Data moves between devices by JAX's collectives and lax.ppermute only.
A program may use at most 64 MiB of HBM per device.

```python
import math
import jax
import jax.numpy as jnp
import numpy as np
from jax import lax

DMAX = 1024
MB = 4
ROWS = 128
REPLICAS = 16
TOTAL_SLOTS = 24
ROWS_ALL = 1024
CAP = 12
N_SECTION = 4
N_REP = 8


def draw_widths(key, part):
    units = jax.random.randint(key, (REPLICAS,), 4, 9)
    return (units * (DMAX // 8)).astype(jnp.int32)


def draw_placement(key, part):
    shuffled = jax.random.permutation(key, TOTAL_SLOTS)
    return shuffled[:REPLICAS].astype(jnp.int32)


def block_levels(rng, extent, shards, smallest, high):
    factor_of, own = 1.0, jax.random.fold_in(rng, 6)
    for axis_at, blocks in shards:
        steps = jnp.exp(jax.random.uniform(jax.random.fold_in(own, axis_at), (blocks,), jnp.float32, smallest / len(shards), high / len(shards)))
        factor_of = factor_of * jnp.repeat(steps, extent[axis_at] // blocks).reshape([-1 if axis == axis_at else 1 for axis in range(len(extent))])
    return factor_of


def assign_block(rng, own, number, rows, number_of, top, most, slope):
    order = jax.random.permutation(rng, number_of)
    crowded, usual = portions_of(number_of, rows * top, most, slope, True), portions_of(number_of, rows * top, most, slope, False)
    places = jnp.arange(number_of)

    def named(sizes, offset_by):
        used = int((sizes > 0).sum())
        fixed = max(1, used // 4)
        shifted = fixed + (places - fixed + offset_by * (used - fixed)) % max(1, number_of - fixed)
        return jnp.zeros((number_of,), jnp.int32).at[order[jnp.where(places < fixed, places, shifted)]].set(jnp.asarray(sizes, jnp.int32))

    sizes = jnp.where(number % 4 == 0, named(crowded, number // 4), named(usual, number - number // 4 - 1))
    mixed = jax.random.permutation(jax.random.fold_in(own, 3), number_of)
    source_of, receiver = mixed[0:number_of // 2 * 2:2], mixed[1:number_of // 2 * 2:2]
    room = jnp.minimum(sizes[source_of] - 1, most - sizes[receiver]) // 2
    room = jnp.where((source_of == order[0]) | (receiver == order[0]) | (sizes[receiver] == 0), 0, jnp.maximum(room, 0))
    shifted = jax.random.randint(jax.random.fold_in(own, 4), (number_of // 2,), 0, 1 << 20) % (room + 1)
    sizes = sizes.at[source_of].add(-shifted).at[receiver].add(shifted)
    items = jnp.searchsorted(jnp.cumsum(sizes), jnp.arange(rows * top), side="right").astype(jnp.int32)
    table = items.reshape(top, rows).T
    table = table[jax.random.permutation(jax.random.fold_in(own, 1), rows)]
    offset_by = jax.random.randint(jax.random.fold_in(own, 2), (rows, 1), 0, top)
    return jnp.take_along_axis(table, (jnp.arange(top)[None, :] + offset_by) % top, axis=1)


def portions_of(amount, total, most, slope, full):
    loads = [(1 << 20) // math.isqrt(grade ** slope) + 1 for grade in range(1, amount + 1)]
    largest = most if full else min(most, max(-(-total // amount), total * loads[0] // sum(loads)))
    least = 1 if total - largest >= amount - 1 else 0
    given, surplus = [largest] + [least] * (amount - 1), total - largest - least * (amount - 1)
    while surplus > 0:
        free = [i for i in range(1, amount) if given[i] < largest] or [i for i in range(1, amount) if given[i] < most]
        mass, left = sum([loads[i] for i in free]), surplus
        for i in free:
            more = min(most - given[i], max(1, left * loads[i] // mass), surplus)
            given[i] = given[i] + more
            surplus = surplus - more
    return np.array(given)


def scatter_about(stream_key, dims, spread, reach, pieces=(), kind=jnp.bfloat16):
    drawn = jax.random.normal(stream_key, dims, jnp.float32) * spread
    if len(pieces) > 0:
        drawn = block_levels(stream_key, dims, pieces, -0.22, 0.18) * drawn
    return jnp.clip(drawn, min=-reach, max=reach).astype(kind)


def setup_inputs(seed: int = 0) -> dict:
    seeds = jax.random.split(jax.random.key(seed), 7)
    tokens = scatter_about(seeds[0], (MB, ROWS_ALL, DMAX), 1.0, 6.0, ((1, 8),))
    replica_of_row_keys = jax.random.split(jax.random.fold_in(seeds[1], 1), MB * ROWS_ALL // ROWS)
    replica_of_row_turns = jax.random.permutation(jax.random.fold_in(seeds[1], 3), MB * ROWS_ALL // ROWS)
    replica_of_row = jax.vmap(lambda own, number: assign_block(jax.random.fold_in(seeds[1], 2), own, number, ROWS, REPLICAS, 1, CAP, 2))(replica_of_row_keys, replica_of_row_turns).reshape((MB, ROWS_ALL, 1))
    widths = draw_widths(jax.random.fold_in(seeds[6], 71), 0)
    placement = draw_placement(jax.random.fold_in(seeds[6], 71), 0)
    gains = jnp.clip(1.0 + 0.1 * jax.random.normal(seeds[4], (N_SECTION, TOTAL_SLOTS, DMAX), jnp.float32), 0.5, 1.5)
    weights = scatter_about(seeds[5], (N_SECTION, TOTAL_SLOTS, DMAX, DMAX), DMAX ** -0.5, 0.1875, ((0, 4), (1, 8)))
    return dict(tokens=tokens, replica_of_row=replica_of_row, widths=widths, placement=placement, gains=gains, weights=weights)


epsilon = 1e-05

def replica_layer(block, weight, gain, width):
    features = jnp.arange(block.shape[1], dtype=jnp.int32)
    is_live = (features < width).astype(jnp.float32)
    float_rows = block.astype(jnp.float32)
    mean_square = lax.optimization_barrier(jnp.sum(float_rows * float_rows, axis=1)) / width.astype(jnp.float32)
    lowered = (float_rows * lax.rsqrt(mean_square + epsilon)[:, None] * gain[None, :]).astype(jnp.bfloat16)
    projected = jnp.dot(lowered, weight, preferred_element_type=jnp.float32)
    return (float_rows + jax.nn.silu(projected) * is_live[None, :]).astype(jnp.bfloat16)

def apply_item(item):
    return replica_layer(item[0], item[1], item[2], item[3])

def reference(tokens, replica_of_row, widths, placement, gains, weights):
    batches, row_total, width_max = tokens.shape
    total = batches * row_total
    row_replica = replica_of_row.reshape(total).astype(jnp.int32)
    features = jnp.arange(width_max, dtype=jnp.int32)
    row_width = widths[row_replica]
    hidden = jnp.where(features[None, :] < row_width[:, None], tokens.reshape(total, width_max), jnp.zeros((), jnp.bfloat16))
    replica_ids = jnp.arange(REPLICAS, dtype=jnp.int32)
    counts = lax.optimization_barrier(jnp.sum((row_replica[None, :] == replica_ids[:, None]).astype(jnp.int32), axis=1))
    order = jnp.argsort(row_replica, stable=True).astype(jnp.int32)
    starts = jnp.cumsum(counts).astype(jnp.int32) - counts
    bound = batches * N_REP * CAP
    offsets = jnp.arange(bound, dtype=jnp.int32)
    position = jnp.clip(starts[:, None] + offsets[None, :], 0, total - 1).astype(jnp.int32)
    gather_index = jnp.where(offsets[None, :] < counts[:, None], order[position], total).astype(jnp.int32)
    for layer in range(N_SECTION):
        padded = jnp.concatenate([hidden, jnp.zeros((1, width_max), jnp.bfloat16)], axis=0)
        grouped = padded[gather_index]
        layer_weights = weights[layer][placement]
        layer_gains = gains[layer][placement]
        updated = lax.map(apply_item, (grouped, layer_weights, layer_gains, widths))
        hidden = hidden.at[gather_index.reshape(-1)].set(updated.reshape(-1, width_max), mode='drop')
    return hidden.reshape(batches, row_total, width_max)
```

```python
import functools
import jax
import jax.numpy as jnp
from jax import lax
from jax.experimental import pallas as pl
from jax.experimental.pallas import tpu as pltpu
from jax.sharding import PartitionSpec as P

epsilon = 1e-05
STREAMS = 2
VMEM_LIMIT = 40 * 1024 * 1024


def earlier_same(first, second, at):
    rows = lax.broadcasted_iota(jnp.int32, (first.shape[0], second.shape[1]), 0)
    lanes = lax.broadcasted_iota(jnp.int32, (first.shape[0], second.shape[1]), 1)
    before = rows < lanes if at == 1 else lanes < rows
    return jnp.where((first == second) & before, 1, 0)


def targets(ids, other, at, table, batch, capacity):
    position = jnp.sum(
        earlier_same(other, ids, 1) if at == 1 else earlier_same(ids, other, 0),
        axis=0 if at == 1 else 1,
        keepdims=True,
    )
    base = jnp.zeros_like(ids)
    for replica, start in enumerate(table):
        base = jnp.where(ids == replica, start, base)
    return base + position + batch * capacity


def start_table(placement, me, slot_count, batches, capacity):
    slot_rows = batches * capacity
    found = []
    for replica in range(placement.shape[0]):
        slot = placement[replica]
        holder = lax.div(slot, slot_count)
        within = slot - holder * slot_count
        found.append((holder ^ me) * (slot_count * slot_rows) + within * slot_rows)
    return found


def dispatch_kernel(sizes, me, placement, lane_ids, row_ids, tokens, *chunks):
    batches, row_count, slot_count, capacity = sizes
    table = start_table(placement, me[0], slot_count, batches, capacity)
    target = jnp.concatenate(
        [
            targets(lane_ids[m], row_ids[m], 1, table, m, capacity)
            for m in range(batches)
        ],
        axis=1,
    )
    slot_rows = batches * capacity
    chunk_rows = slot_count * slot_rows
    source = jnp.concatenate([tokens[m] for m in range(batches)], axis=0)
    for i, chunk in enumerate(chunks):
        wanted = lax.broadcasted_iota(jnp.int32, (chunk_rows, batches * row_count), 0)
        picked = jnp.where(target == wanted + i * chunk_rows, 1.0, 0.0).astype(jnp.bfloat16)
        moved = jnp.dot(picked, source, preferred_element_type=jnp.float32).astype(jnp.bfloat16)
        for j in range(slot_count):
            chunk[j] = moved[j * slot_rows : (j + 1) * slot_rows]


def combine_kernel(sizes, me, placement, lane_ids, row_ids, returned, out):
    batches, row_count, slot_count, capacity = sizes
    table = start_table(placement, me[0], slot_count, batches, capacity)
    chunk_count = returned.shape[0]
    flat = jnp.concatenate(
        [returned[i, j] for i in range(chunk_count) for j in range(slot_count)], axis=0
    )
    for m in range(batches):
        target = targets(row_ids[m], lane_ids[m], 0, table, m, capacity)
        held = lax.broadcasted_iota(jnp.int32, (row_count, flat.shape[0]), 1)
        picked = jnp.where(target == held, 1.0, 0.0).astype(jnp.bfloat16)
        out[m] = jnp.dot(picked, flat, preferred_element_type=jnp.float32).astype(jnp.bfloat16)


def layer_kernel(two, is_first, width, scale, *refs):
    if two:
        first, arrived, gain, weight, out = refs
        rows = jnp.where(is_first[0] == 1, first[0], arrived[0]).astype(jnp.float32)
    else:
        arrived, gain, weight, out = refs
        rows = arrived[0].astype(jnp.float32)
    slot = pl.program_id(0)
    live = lax.broadcasted_iota(jnp.int32, (1, rows.shape[1]), 1) < width[slot]
    rows = jnp.where(live, rows, 0.0)
    mean_square = jnp.sum(rows * rows, axis=1, keepdims=True) * scale[slot]
    lowered = (rows * lax.rsqrt(mean_square + epsilon) * gain[0]).astype(jnp.bfloat16)
    projected = jnp.dot(lowered, weight[0], preferred_element_type=jnp.float32)
    gate = projected * jax.nn.sigmoid(projected)
    out[0] = (rows + jnp.where(live, gate, 0.0)).astype(jnp.bfloat16)


def layer(first, arrived, is_first, width, scale, gain, weight):
    given = [a for a in (first, arrived) if a is not None]
    slot_count, slot_rows, depth = given[0].shape
    smem = pl.BlockSpec(memory_space=pltpu.SMEM)
    block = pl.BlockSpec((1, slot_rows, depth), lambda j: (j, 0, 0))
    return pl.pallas_call(
        functools.partial(layer_kernel, len(given) == 2),
        grid=(slot_count,),
        in_specs=[smem] * 3
        + [block] * len(given)
        + [
            pl.BlockSpec((1, 1, depth), lambda j: (j, 0, 0)),
            pl.BlockSpec((1, depth, depth), lambda j: (j, 0, 0)),
        ],
        out_specs=block,
        out_shape=jax.ShapeDtypeStruct(given[0].shape, jnp.bfloat16),
        compiler_params=pltpu.CompilerParams(vmem_limit_bytes=VMEM_LIMIT),
        cost_estimate=pl.CostEstimate(
            flops=2 * slot_count * slot_rows * depth * depth,
            bytes_accessed=2 * slot_count * depth * (depth + 3 * slot_rows),
            transcendentals=0,
        ),
        name="layer",
    )(is_first, width, scale, *given, gain, weight)


def on_device(tokens, replica_of_row, widths, placement, gains, weights):
    batches, row_count, depth = tokens.shape
    rep_count = lax.axis_size("rep")
    section_count = lax.axis_size("section")
    slot_count = weights.shape[1]
    replica_count = widths.shape[0]
    capacity = (3 * row_count + 2 * replica_count - 1) // (2 * replica_count)
    section_id = lax.axis_index("section")
    rep_id = lax.axis_index("rep")
    last = section_count - 1
    part = depth // section_count
    slot_rows = batches * capacity

    global_ids = rep_id * slot_count + jnp.arange(slot_count, dtype=jnp.int32)
    width = jnp.sum(
        jnp.where(placement[None, :] == global_ids[:, None], widths[None, :], 0), axis=1
    )
    scale = 1.0 / jnp.maximum(width, 1).astype(jnp.float32)
    is_first = (section_id == 0).astype(jnp.int32).reshape(1)
    me = rep_id.astype(jnp.int32).reshape(1)
    gain = gains.reshape(slot_count, 1, depth)
    weight = weights.reshape(slot_count, depth, depth)
    lane_ids = replica_of_row.reshape(batches, 1, row_count)

    sizes = (batches, row_count, slot_count, capacity)
    smem = pl.BlockSpec(memory_space=pltpu.SMEM)
    vmem = pl.BlockSpec(memory_space=pltpu.VMEM)
    chunk_shape = jax.ShapeDtypeStruct((slot_count, slot_rows, depth), jnp.bfloat16)
    outgoing = pl.pallas_call(
        functools.partial(dispatch_kernel, sizes),
        in_specs=[smem, smem, vmem, vmem, vmem],
        out_specs=[vmem] * rep_count,
        out_shape=[chunk_shape] * rep_count,
        compiler_params=pltpu.CompilerParams(vmem_limit_bytes=VMEM_LIMIT),
        name="dispatch",
    )(me, placement, lane_ids, replica_of_row, tokens)

    def traded(x, i):
        if i == 0:
            return x
        return lax.ppermute(x, "rep", [(d, d ^ i) for d in range(rep_count)])

    entering = [traded(outgoing[i], i) for i in range(rep_count)]
    forward = [(s, s + 1) for s in range(last)]
    lag = STREAMS * last
    inbound, finished = {}, []
    for n in range(rep_count + lag):
        first = entering[n] if n < rep_count else None
        arrived = inbound.get(n)
        done = layer(first, arrived, is_first, width, scale, gain, weight)
        if n < rep_count + lag - STREAMS:
            inbound[n + STREAMS] = lax.ppermute(done, "section", forward)
        if n >= lag:
            finished.append(done)

    half, quarter = rep_count // 2, rep_count // 4
    pieces = []
    for low, high in ((0, half), (half, half + quarter), (half + quarter, rep_count)):
        group = jnp.stack(finished[low:high])
        mine = group[..., last * part :]
        for s in range(last):
            sent = lax.ppermute(group[..., s * part : (s + 1) * part], "section", [(last, s)])
            mine = jnp.where(section_id == s, sent, mine)
        pieces.append(mine)
    held = jnp.concatenate(pieces)
    by_owner = jnp.stack(
        [lax.dynamic_index_in_dim(held, rep_id ^ b, 0, keepdims=False) for b in range(rep_count)]
    )
    returned = lax.all_to_all(by_owner, "rep", split_axis=0, concat_axis=0, tiled=True)
    zero = jnp.zeros((1,), jnp.int32)
    return pl.pallas_call(
        functools.partial(combine_kernel, sizes),
        in_specs=[smem, smem, vmem, vmem, vmem],
        out_specs=vmem,
        out_shape=jax.ShapeDtypeStruct((batches, row_count, part), jnp.bfloat16),
        compiler_params=pltpu.CompilerParams(vmem_limit_bytes=VMEM_LIMIT),
        name="combine",
    )(zero, placement, lane_ids, replica_of_row, returned)


def solution(mesh):
    placed = (
        P(None, "rep", None),
        P(None, "rep", None),
        P(),
        P(),
        P("section", "rep", None),
        P("section", "rep", None, None),
    )
    return jax.shard_map(
        on_device, mesh=mesh, in_specs=placed, out_specs=P(None, "rep", "section"), check_vma=False
    )
```

```python
import functools
import jax
import jax.numpy as jnp
from jax import lax
from jax.experimental import pallas as pl
from jax.experimental.pallas import tpu as pltpu
from jax.sharding import PartitionSpec as P

epsilon = 1e-05
STREAMS = 2
SMALL_VMEM = 12 * 1024 * 1024
VMEM_LIMIT = 24 * 1024 * 1024

ANY = pl.BlockSpec(memory_space=pl.ANY)
SMEM = pl.BlockSpec(memory_space=pltpu.SMEM)
VMEM = pl.BlockSpec(memory_space=pltpu.VMEM)


def upright(row):
    return jnp.transpose(jnp.broadcast_to(row, (row.shape[1], row.shape[1])))


def open_kernel(out):
    out[...] = jnp.zeros_like(out)


def dispatch_kernel(sizes, placement, widths, ids, tokens, gains, opened, target, table, *chunks):
    batches, row_count, slot_count, capacity, depth = sizes
    me = lax.axis_index("rep")
    slot_rows = batches * capacity
    replica_count = placement.shape[0]
    starts, slots = [], []
    for replica in range(replica_count):
        slot = placement[replica]
        holder = lax.div(slot, slot_count)
        starts.append(((holder ^ me) * slot_count + slot - holder * slot_count) * slot_rows)
        slots.append(slot)
    features = lax.broadcasted_iota(jnp.int32, (1, depth), 1)
    for j in range(slot_count):
        width = jnp.int32(0)
        for replica in range(replica_count):
            width = width + jnp.where(slots[replica] == me * slot_count + j, widths[replica], 0)
        inverse = 1.0 / jnp.maximum(jnp.full((1, depth), width), 1).astype(jnp.float32)
        table[j, 0:1] = gains[j]
        table[j, 1:2] = jnp.where(features < width, inverse, 0.0)

    square = (row_count, row_count)
    early = lax.broadcasted_iota(jnp.int32, square, 0) < lax.broadcasted_iota(jnp.int32, square, 1)
    rows = []
    for m in range(batches):
        own = ids[m]
        same = jnp.where((upright(own) == own) & early, 1, 0)
        row = jnp.sum(same, axis=0, keepdims=True) + m * capacity
        for replica, start in enumerate(starts):
            row = row + jnp.where(own == replica, start, 0)
        target[m] = row
        rows.append(row)
    row = jnp.concatenate(rows, axis=1)
    chunk_rows = slot_count * slot_rows
    source = jnp.concatenate([tokens[m] for m in range(batches)], axis=0)
    for i, chunk in enumerate(chunks):
        wanted = lax.broadcasted_iota(jnp.int32, (chunk_rows, batches * row_count), 0)
        picked = jnp.where(row == wanted + i * chunk_rows, 1.0, 0.0).astype(jnp.bfloat16)
        moved = jnp.dot(picked, source, preferred_element_type=jnp.float32).astype(jnp.bfloat16)
        for j in range(slot_count):
            chunk[j] = moved[j * slot_rows : (j + 1) * slot_rows]


def route_kernel(target, token, picked):
    for m in range(picked.shape[0]):
        wanted = upright(target[m])[:, :1]
        place = lax.broadcasted_iota(jnp.int32, picked.shape[1:], 1)
        picked[m] = jnp.where(wanted == place, 1.0, 0.0).astype(jnp.bfloat16)


def layer_kernel(has_first, has_arrived, before_count, forwards, parts, *refs):
    refs = list(refs)
    first = refs.pop(0) if has_first else None
    arrived = refs.pop(0) if has_arrived else None
    before = [refs.pop(0) for _ in range(before_count)]
    table, weight, _ = refs[:3]
    outs = refs[3:]
    if first is not None and arrived is not None:
        rows = jnp.where(lax.axis_index("section") == 0, first[0], arrived[0])
    else:
        rows = first[0] if arrived is None else arrived[0]
    rows = rows.astype(jnp.float32)
    gain, inverse = table[0, 0:1], table[0, 1:2]
    rows = jnp.where(inverse > 0.0, rows, 0.0)
    mean_square = jnp.sum(rows * rows * inverse, axis=1, keepdims=True)
    lowered = (rows * lax.rsqrt(mean_square + epsilon) * gain).astype(jnp.bfloat16)
    projected = jnp.dot(lowered, weight[0], preferred_element_type=jnp.float32)
    gate = projected * jax.nn.sigmoid(projected)
    done = (rows + jnp.where(inverse > 0.0, gate, 0.0)).astype(jnp.bfloat16)
    if forwards:
        outs.pop(0)[0] = done
    for s in range(parts):
        size = done.shape[1] // parts
        for at, ref in enumerate(before):
            outs[s][at, 0] = ref[0, :, s * size : (s + 1) * size]
        outs[s][before_count, 0] = done[:, s * size : (s + 1) * size]


def layer(first, arrived, before, token, table, weight, forwards, parts, held):
    given = [a for a in (first, arrived) if a is not None] + before
    slot_count, slot_rows, depth = given[0].shape
    block = pl.BlockSpec((1, slot_rows, depth), lambda j: (j, 0, 0))
    out_specs, out_shape = [], []
    if forwards:
        out_specs.append(block)
        out_shape.append(jax.ShapeDtypeStruct(given[0].shape, jnp.bfloat16))
    for _ in range(parts):
        size = depth // parts
        out_specs.append(pl.BlockSpec((held, 1, slot_rows, size), lambda j: (0, j, 0, 0)))
        out_shape.append(
            jax.ShapeDtypeStruct((held, slot_count, slot_rows, size), jnp.bfloat16)
        )
    return pl.pallas_call(
        functools.partial(
            layer_kernel, first is not None, arrived is not None, len(before), forwards, parts
        ),
        grid=(slot_count,),
        in_specs=[block] * len(given)
        + [
            pl.BlockSpec((1, 2, depth), lambda j: (j, 0, 0)),
            pl.BlockSpec((1, depth, depth), lambda j: (j, 0, 0)),
            ANY,
        ],
        out_specs=out_specs,
        out_shape=out_shape,
        compiler_params=pltpu.CompilerParams(vmem_limit_bytes=SMALL_VMEM),
        cost_estimate=pl.CostEstimate(
            flops=2 * slot_count * slot_rows * depth * depth,
            bytes_accessed=2 * slot_count * depth * (depth + 3 * slot_rows),
            transcendentals=0,
        ),
        name="layer",
    )(*given, table, weight, token)


def chosen(candidates):
    section = lax.axis_index("section")
    value = candidates[0]
    for s in range(1, len(candidates)):
        value = jnp.where(section == s, candidates[s], value)
    return value


def pick_kernel(sections, groups, token, *refs):
    outs = list(refs[sections * len(groups) :])
    for g, group in enumerate(groups):
        mine = refs[g * sections : (g + 1) * sections]
        for h in range(len(group)):
            out = outs.pop(0)
            for j in range(out.shape[0]):
                out[j] = chosen([ref[h, j] for ref in mine])


def combine_kernel(sections, direct, spans, picked, acc, *refs):
    out, refs = refs[-1], refs[:-1]
    rows = []
    for at in range(len(spans)):
        mine = refs[at * sections : (at + 1) * sections] if direct else refs[at : at + 1]
        for j in range(mine[0].shape[1] if direct else mine[0].shape[0]):
            rows.append(chosen([ref[0, j] for ref in mine]) if direct else mine[0][j])
    flat = jnp.concatenate(rows, axis=0)
    for m in range(out.shape[0]):
        select = jnp.concatenate([picked[m, :, low:high] for low, high in spans], axis=1)
        value = jnp.dot(select, flat, preferred_element_type=jnp.float32)
        if acc is not None:
            value = value + acc[m]
        out[m] = value.astype(out.dtype)


def schedule(rep_count):
    order = [0, 1, 4, 3, 5] + list(range(6, rep_count)) + [2]
    early = order[:-2]
    size = max(3, -(-len(early) // 4))
    groups = [early[at : at + size] for at in range(0, len(early), size)]
    return order, groups, order[-2:]


def on_device(tokens, replica_of_row, widths, placement, gains, weights):
    batches, row_count, depth = tokens.shape
    rep_count = lax.axis_size("rep")
    section_count = lax.axis_size("section")
    slot_count = weights.shape[1]
    replica_count = widths.shape[0]
    capacity = (3 * row_count + 2 * replica_count - 1) // (2 * replica_count)
    last = section_count - 1
    part = depth // section_count
    slot_rows = batches * capacity
    chunk_rows = slot_count * slot_rows

    gain = gains.reshape(slot_count, 1, depth)
    weight = weights.reshape(slot_count, depth, depth)
    ids = replica_of_row.reshape(batches, 1, row_count)
    chunk_shape = jax.ShapeDtypeStruct((slot_count, slot_rows, depth), jnp.bfloat16)
    opened = pl.pallas_call(
        open_kernel,
        in_specs=[],
        out_specs=VMEM,
        out_shape=jax.ShapeDtypeStruct((8, 128), jnp.float32),
        compiler_params=pltpu.CompilerParams(vmem_limit_bytes=1024 * 1024),
        cost_estimate=pl.CostEstimate(
            flops=16 * 1024**3, bytes_accessed=64 * 1024**2, transcendentals=0
        ),
        name="open",
    )()
    target, table, *outgoing = pl.pallas_call(
        functools.partial(
            dispatch_kernel, (batches, row_count, slot_count, capacity, depth)
        ),
        in_specs=[SMEM, SMEM, VMEM, VMEM, VMEM, ANY],
        out_specs=[VMEM] * (rep_count + 2),
        out_shape=[
            jax.ShapeDtypeStruct(ids.shape, jnp.int32),
            jax.ShapeDtypeStruct((slot_count, 2, depth), jnp.float32),
        ]
        + [chunk_shape] * rep_count,
        compiler_params=pltpu.CompilerParams(vmem_limit_bytes=VMEM_LIMIT),
        cost_estimate=pl.CostEstimate(
            flops=2 * batches * row_count * rep_count * chunk_rows * depth,
            bytes_accessed=2 * depth * (batches * row_count + rep_count * chunk_rows),
            transcendentals=0,
        ),
        name="dispatch",
    )(placement, widths, ids, tokens, gain, opened)

    def traded(x, i):
        if i == 0:
            return x
        return lax.ppermute(x, "rep", [(d, d ^ i) for d in range(rep_count)])

    order, groups, direct = schedule(rep_count)

    def arriving(x, i):
        if i == 0:
            return x
        return lax.ppermute(x, ("section", "rep"), [(d, d ^ i) for d in range(rep_count)])

    entering = {i: arriving(outgoing[i], i) for i in order}

    def sent_back(pieces, hop):
        sent = []
        for s, piece in enumerate(pieces):
            if s != last or hop != 0:
                hops = [(last * rep_count + d, s * rep_count + (d ^ hop)) for d in range(rep_count)]
                piece = lax.ppermute(piece, ("section", "rep"), hops)
            sent.append(piece)
        return sent

    lag = STREAMS * last
    inbound, finished, back = {}, {}, {}
    token = target
    picked = None
    for n in range(rep_count + lag):
        first = entering[order[n]] if n < rep_count else None
        arrived = inbound.get(n)
        closing = groups + [[i] for i in direct]
        group = next((g for g in closing if n >= lag and g[-1] == order[n - lag]), None)
        before = [finished[i] for i in group[:-1]] if group else []
        opens = n >= lag and group is None
        forward = [(s, s + 1) for s in range(last) if 0 <= n - STREAMS * s < rep_count]
        forwards = n < rep_count + lag - STREAMS or opens
        made = layer(
            first,
            arrived,
            before,
            token,
            table,
            weight,
            forwards,
            section_count if group else 0,
            len(group) if group else 0,
        )
        token = made[0]
        if n < rep_count + lag - STREAMS:
            inbound[n + STREAMS] = lax.ppermute(made[0], "section", forward)
        if opens:
            finished[order[n - lag]] = made[0]
        if group:
            hop = group[0] if group[0] in direct else 0
            back[group[0]] = sent_back(made[-section_count:], hop)
        if n == 1:
            token = picked = pl.pallas_call(
                route_kernel,
                in_specs=[VMEM, ANY],
                out_specs=VMEM,
                out_shape=jax.ShapeDtypeStruct(
                    (batches, row_count, rep_count * chunk_rows), jnp.bfloat16
                ),
                compiler_params=pltpu.CompilerParams(vmem_limit_bytes=SMALL_VMEM),
                name="route",
            )(target, token)

    mine = pl.pallas_call(
        functools.partial(pick_kernel, section_count, groups),
        in_specs=[ANY] + [VMEM] * (section_count * len(groups)),
        out_specs=[VMEM] * (rep_count - len(direct)),
        out_shape=[jax.ShapeDtypeStruct((slot_count, slot_rows, part), jnp.bfloat16)]
        * (rep_count - len(direct)),
        compiler_params=pltpu.CompilerParams(vmem_limit_bytes=SMALL_VMEM),
        name="pick",
    )(token, *[piece for group in groups for piece in back[group[0]]])
    early = order[: len(mine)]
    returned = [traded(piece, i) for i, piece in zip(early, mine)]

    def combined(these, acc, given, dtype, is_direct):
        spans = [(i * chunk_rows, (i + 1) * chunk_rows) for i in these]

        def kernel(picked, *refs):
            refs = list(refs)
            some = refs.pop(0) if acc is not None else None
            combine_kernel(section_count, is_direct, spans, picked, some, *refs)

        extra = [] if acc is None else [acc]
        return pl.pallas_call(
            kernel,
            in_specs=[VMEM] * (1 + len(extra) + len(given)),
            out_specs=VMEM,
            out_shape=jax.ShapeDtypeStruct((batches, row_count, part), dtype),
            compiler_params=pltpu.CompilerParams(vmem_limit_bytes=SMALL_VMEM),
            name="combine",
        )(picked, *extra, *given)

    acc = combined(early, None, returned, jnp.float32, False)
    late = [piece for i in direct for piece in back[i]]
    return combined(direct, acc, late, jnp.bfloat16, True)


def solution(mesh):
    placed = (
        P(None, "rep", None),
        P(None, "rep", None),
        P(),
        P(),
        P("section", "rep", None),
        P("section", "rep", None, None),
    )

    return jax.shard_map(
        on_device, mesh=mesh, in_specs=placed, out_specs=P(None, "rep", "section"), check_vma=False
    )
```

```python
import functools
import jax
import jax.numpy as jnp
from jax import lax
from jax.experimental import pallas as pl
from jax.experimental.pallas import tpu as pltpu
from jax.sharding import PartitionSpec as P

epsilon = 1e-05
STREAMS = 2
SMALL_VMEM = 12 * 1024 * 1024
VMEM_LIMIT = 24 * 1024 * 1024

ANY = pl.BlockSpec(memory_space=pl.ANY)
SMEM = pl.BlockSpec(memory_space=pltpu.SMEM)
VMEM = pl.BlockSpec(memory_space=pltpu.VMEM)


def upright(row):
    return jnp.transpose(jnp.broadcast_to(row, (row.shape[1], row.shape[1])))


def open_kernel(out):
    out[...] = jnp.zeros_like(out)


def dispatch_kernel(sizes, placement, widths, ids, tokens, gains, opened, target, table, *chunks):
    batches, row_count, slot_count, capacity, depth = sizes
    me = lax.axis_index("rep")
    slot_rows = batches * capacity
    replica_count = placement.shape[0]
    starts, slots = [], []
    for replica in range(replica_count):
        slot = placement[replica]
        holder = lax.div(slot, slot_count)
        starts.append(((holder ^ me) * slot_count + slot - holder * slot_count) * slot_rows)
        slots.append(slot)
    features = lax.broadcasted_iota(jnp.int32, (1, depth), 1)
    for j in range(slot_count):
        width = jnp.int32(0)
        for replica in range(replica_count):
            width = width + jnp.where(slots[replica] == me * slot_count + j, widths[replica], 0)
        inverse = 1.0 / jnp.maximum(jnp.full((1, depth), width), 1).astype(jnp.float32)
        table[j, 0:1] = gains[j]
        table[j, 1:2] = jnp.where(features < width, inverse, 0.0)

    square = (row_count, row_count)
    early = lax.broadcasted_iota(jnp.int32, square, 0) < lax.broadcasted_iota(jnp.int32, square, 1)
    rows = []
    for m in range(batches):
        own = ids[m]
        same = jnp.where((upright(own) == own) & early, 1, 0)
        row = jnp.sum(same, axis=0, keepdims=True) + m * capacity
        for replica, start in enumerate(starts):
            row = row + jnp.where(own == replica, start, 0)
        target[m] = row
        rows.append(row)
    row = jnp.concatenate(rows, axis=1)
    chunk_rows = slot_count * slot_rows
    source = jnp.concatenate([tokens[m] for m in range(batches)], axis=0)
    for i, chunk in enumerate(chunks):
        wanted = lax.broadcasted_iota(jnp.int32, (chunk_rows, batches * row_count), 0)
        picked = jnp.where(row == wanted + i * chunk_rows, 1.0, 0.0).astype(jnp.bfloat16)
        moved = jnp.dot(picked, source, preferred_element_type=jnp.float32).astype(jnp.bfloat16)
        for j in range(slot_count):
            chunk[j] = moved[j * slot_rows : (j + 1) * slot_rows]


def route_kernel(target, token, picked):
    for m in range(picked.shape[0]):
        wanted = upright(target[m])[:, :1]
        place = lax.broadcasted_iota(jnp.int32, picked.shape[1:], 1)
        picked[m] = jnp.where(wanted == place, 1.0, 0.0).astype(jnp.bfloat16)


def layer_kernel(has_first, has_arrived, before_count, forwards, parts, *refs):
    refs = list(refs)
    first = refs.pop(0) if has_first else None
    arrived = refs.pop(0) if has_arrived else None
    before = [refs.pop(0) for _ in range(before_count)]
    table, weight, _ = refs[:3]
    outs = refs[3:]
    if first is not None and arrived is not None:
        rows = jnp.where(lax.axis_index("section") == 0, first[0], arrived[0])
    else:
        rows = first[0] if arrived is None else arrived[0]
    rows = rows.astype(jnp.float32)
    gain, inverse = table[0, 0:1], table[0, 1:2]
    rows = jnp.where(inverse > 0.0, rows, 0.0)
    mean_square = jnp.sum(rows * rows * inverse, axis=1, keepdims=True)
    lowered = (rows * lax.rsqrt(mean_square + epsilon) * gain).astype(jnp.bfloat16)
    projected = jnp.dot(lowered, weight[0], preferred_element_type=jnp.float32)
    gate = projected * jax.nn.sigmoid(projected)
    done = (rows + jnp.where(inverse > 0.0, gate, 0.0)).astype(jnp.bfloat16)
    if forwards:
        outs.pop(0)[0] = done
    for s in range(parts):
        size = done.shape[1] // parts
        for at, ref in enumerate(before):
            outs[s][at, 0] = ref[0, :, s * size : (s + 1) * size]
        outs[s][before_count, 0] = done[:, s * size : (s + 1) * size]


def layer(first, arrived, before, token, table, weight, forwards, parts, held):
    given = [a for a in (first, arrived) if a is not None] + before
    slot_count, slot_rows, depth = given[0].shape
    block = pl.BlockSpec((1, slot_rows, depth), lambda j: (j, 0, 0))
    out_specs, out_shape = [], []
    if forwards:
        out_specs.append(block)
        out_shape.append(jax.ShapeDtypeStruct(given[0].shape, jnp.bfloat16))
    for _ in range(parts):
        size = depth // parts
        out_specs.append(pl.BlockSpec((held, 1, slot_rows, size), lambda j: (0, j, 0, 0)))
        out_shape.append(
            jax.ShapeDtypeStruct((held, slot_count, slot_rows, size), jnp.bfloat16)
        )
    return pl.pallas_call(
        functools.partial(
            layer_kernel, first is not None, arrived is not None, len(before), forwards, parts
        ),
        grid=(slot_count,),
        in_specs=[block] * len(given)
        + [
            pl.BlockSpec((1, 2, depth), lambda j: (j, 0, 0)),
            pl.BlockSpec((1, depth, depth), lambda j: (j, 0, 0)),
            ANY,
        ],
        out_specs=out_specs,
        out_shape=out_shape,
        compiler_params=pltpu.CompilerParams(vmem_limit_bytes=SMALL_VMEM),
        cost_estimate=pl.CostEstimate(
            flops=2 * slot_count * slot_rows * depth * depth,
            bytes_accessed=2 * slot_count * depth * (depth + 3 * slot_rows),
            transcendentals=0,
        ),
        name="layer",
    )(*given, table, weight, token)


def chosen(candidates):
    section = lax.axis_index("section")
    value = candidates[0]
    for s in range(1, len(candidates)):
        value = jnp.where(section == s, candidates[s], value)
    return value


def pick_kernel(sections, groups, token, *refs):
    outs = list(refs[sections * len(groups) :])
    for g, group in enumerate(groups):
        mine = refs[g * sections : (g + 1) * sections]
        for h in range(len(group)):
            out = outs.pop(0)
            for j in range(out.shape[0]):
                out[j] = chosen([ref[h, j] for ref in mine])


def combine_kernel(sections, direct, spans, picked, acc, *refs):
    out, refs = refs[-1], refs[:-1]
    rows = []
    for at in range(len(spans)):
        mine = refs[at * sections : (at + 1) * sections] if direct else refs[at : at + 1]
        for j in range(mine[0].shape[1] if direct else mine[0].shape[0]):
            rows.append(chosen([ref[0, j] for ref in mine]) if direct else mine[0][j])
    flat = jnp.concatenate(rows, axis=0)
    for m in range(out.shape[0]):
        select = jnp.concatenate([picked[m, :, low:high] for low, high in spans], axis=1)
        value = jnp.dot(select, flat, preferred_element_type=jnp.float32)
        if acc is not None:
            value = value + acc[m]
        out[m] = value.astype(out.dtype)


def schedule(rep_count):
    order = [0, 1, 4, 3, 5] + list(range(6, rep_count)) + [2]
    early = order[:-2]
    size = max(3, -(-len(early) // 4))
    groups = [early[at : at + size] for at in range(0, len(early), size)]
    return order, groups, order[-2:]


def on_device(tokens, replica_of_row, widths, placement, gains, weights):
    batches, row_count, depth = tokens.shape
    rep_count = lax.axis_size("rep")
    section_count = lax.axis_size("section")
    slot_count = weights.shape[1]
    replica_count = widths.shape[0]
    capacity = (3 * row_count + 2 * replica_count - 1) // (2 * replica_count)
    last = section_count - 1
    part = depth // section_count
    slot_rows = batches * capacity
    chunk_rows = slot_count * slot_rows

    gain = gains.reshape(slot_count, 1, depth)
    weight = weights.reshape(slot_count, depth, depth)
    ids = replica_of_row.reshape(batches, 1, row_count)
    chunk_shape = jax.ShapeDtypeStruct((slot_count, slot_rows, depth), jnp.bfloat16)
    opened = pl.pallas_call(
        open_kernel,
        in_specs=[],
        out_specs=VMEM,
        out_shape=jax.ShapeDtypeStruct((8, 128), jnp.float32),
        compiler_params=pltpu.CompilerParams(vmem_limit_bytes=1024 * 1024),
        cost_estimate=pl.CostEstimate(
            flops=16 * 1024**3, bytes_accessed=64 * 1024**2, transcendentals=0
        ),
        name="open",
    )()
    target, table, *outgoing = pl.pallas_call(
        functools.partial(
            dispatch_kernel, (batches, row_count, slot_count, capacity, depth)
        ),
        in_specs=[SMEM, SMEM, VMEM, VMEM, VMEM, ANY],
        out_specs=[VMEM] * (rep_count + 2),
        out_shape=[
            jax.ShapeDtypeStruct(ids.shape, jnp.int32),
            jax.ShapeDtypeStruct((slot_count, 2, depth), jnp.float32),
        ]
        + [chunk_shape] * rep_count,
        compiler_params=pltpu.CompilerParams(vmem_limit_bytes=VMEM_LIMIT),
        cost_estimate=pl.CostEstimate(
            flops=2 * batches * row_count * rep_count * chunk_rows * depth,
            bytes_accessed=2 * depth * (batches * row_count + rep_count * chunk_rows),
            transcendentals=0,
        ),
        name="dispatch",
    )(placement, widths, ids, tokens, gain, opened)

    def traded(x, i):
        if i == 0:
            return x
        return lax.ppermute(x, "rep", [(d, d ^ i) for d in range(rep_count)])

    order, groups, direct = schedule(rep_count)

    def arriving(x, i):
        if i == 0:
            return x
        hops = [
            (s * rep_count + d, s * rep_count + (d ^ (i if s == 0 else 1)))
            for s in range(section_count)
            for d in range(rep_count)
        ]
        return lax.ppermute(x, ("section", "rep"), hops)

    entering = {i: arriving(outgoing[i], i) for i in order}

    def sent_back(pieces, hop):
        sent = []
        for s, piece in enumerate(pieces):
            if s != last or hop != 0:
                hops = [(last * rep_count + d, s * rep_count + (d ^ hop)) for d in range(rep_count)]
                if s == last:
                    hops += [
                        (t * rep_count + d, t * rep_count + (d ^ 1))
                        for t in range(last)
                        for d in range(rep_count)
                    ]
                piece = lax.ppermute(piece, ("section", "rep"), hops)
            sent.append(piece)
        return sent

    lag = STREAMS * last
    inbound, finished, back = {}, {}, {}
    token = target
    picked = None
    for n in range(rep_count + lag):
        first = entering[order[n]] if n < rep_count else None
        arrived = inbound.get(n)
        closing = groups + [[i] for i in direct]
        group = next((g for g in closing if n >= lag and g[-1] == order[n - lag]), None)
        before = [finished[i] for i in group[:-1]] if group else []
        opens = n >= lag and group is None
        forward = [(s, s + 1) for s in range(last) if 0 <= n - STREAMS * s < rep_count]
        forwards = n < rep_count + lag - STREAMS or opens
        made = layer(
            first,
            arrived,
            before,
            token,
            table,
            weight,
            forwards,
            section_count if group else 0,
            len(group) if group else 0,
        )
        token = made[0]
        if n < rep_count + lag - STREAMS:
            inbound[n + STREAMS] = lax.ppermute(made[0], "section", forward)
        if opens:
            finished[order[n - lag]] = made[0]
        if group:
            hop = group[0] if group[0] in direct else 0
            back[group[0]] = sent_back(made[-section_count:], hop)
        if n == 1:
            token = picked = pl.pallas_call(
                route_kernel,
                in_specs=[VMEM, ANY],
                out_specs=VMEM,
                out_shape=jax.ShapeDtypeStruct(
                    (batches, row_count, rep_count * chunk_rows), jnp.bfloat16
                ),
                compiler_params=pltpu.CompilerParams(vmem_limit_bytes=SMALL_VMEM),
                name="route",
            )(target, token)

    mine = pl.pallas_call(
        functools.partial(pick_kernel, section_count, groups),
        in_specs=[ANY] + [VMEM] * (section_count * len(groups)),
        out_specs=[VMEM] * (rep_count - len(direct)),
        out_shape=[jax.ShapeDtypeStruct((slot_count, slot_rows, part), jnp.bfloat16)]
        * (rep_count - len(direct)),
        compiler_params=pltpu.CompilerParams(vmem_limit_bytes=SMALL_VMEM),
        name="pick",
    )(token, *[piece for group in groups for piece in back[group[0]]])
    early = order[: len(mine)]
    returned = []
    for i, piece in zip(early, mine):
        returned.append(traded(piece, i))

    def combined(these, acc, given, dtype, is_direct):
        spans = [(i * chunk_rows, (i + 1) * chunk_rows) for i in these]

        def kernel(picked, *refs):
            refs = list(refs)
            some = refs.pop(0) if acc is not None else None
            combine_kernel(section_count, is_direct, spans, picked, some, *refs)

        extra = [] if acc is None else [acc]
        return pl.pallas_call(
            kernel,
            in_specs=[VMEM] * (1 + len(extra) + len(given)),
            out_specs=VMEM,
            out_shape=jax.ShapeDtypeStruct((batches, row_count, part), dtype),
            compiler_params=pltpu.CompilerParams(vmem_limit_bytes=SMALL_VMEM),
            name="combine",
        )(picked, *extra, *given)

    acc = combined(early, None, returned, jnp.float32, False)
    late = [piece for i in direct for piece in back[i]]
    return combined(direct, acc, late, jnp.bfloat16, True)


def solution(mesh):
    placed = (
        P(None, "rep", None),
        P(None, "rep", None),
        P(),
        P(),
        P("section", "rep", None),
        P("section", "rep", None, None),
    )

    return jax.shard_map(
        on_device, mesh=mesh, in_specs=placed, out_specs=P(None, "rep", "section"), check_vma=False
    )
```

```python
import functools
import jax
import jax.numpy as jnp
from jax import lax
from jax.experimental import pallas as pl
from jax.experimental.pallas import tpu as pltpu
from jax.sharding import PartitionSpec as P

epsilon = 1e-05
STREAMS = 2
ALONE = 2
SIZES = (4, 2)
SMALL_VMEM = 12 * 1024 * 1024
VMEM_LIMIT = 24 * 1024 * 1024

ANY = pl.BlockSpec(memory_space=pl.ANY)
SMEM = pl.BlockSpec(memory_space=pltpu.SMEM)
VMEM = pl.BlockSpec(memory_space=pltpu.VMEM)


def upright(row):
    return jnp.transpose(jnp.broadcast_to(row, (row.shape[1], row.shape[1])))


def open_kernel(out):
    out[...] = jnp.zeros_like(out)


def dispatch_kernel(sizes, placement, widths, ids, tokens, gains, opened, target, table, *chunks):
    batches, row_count, slot_count, capacity, depth = sizes
    me = lax.axis_index("rep")
    slot_rows = batches * capacity
    replica_count = placement.shape[0]
    starts, slots = [], []
    for replica in range(replica_count):
        slot = placement[replica]
        holder = lax.div(slot, slot_count)
        starts.append(((holder ^ me) * slot_count + slot - holder * slot_count) * slot_rows)
        slots.append(slot)
    features = lax.broadcasted_iota(jnp.int32, (1, depth), 1)
    for j in range(slot_count):
        width = jnp.int32(0)
        for replica in range(replica_count):
            width = width + jnp.where(slots[replica] == me * slot_count + j, widths[replica], 0)
        inverse = 1.0 / jnp.maximum(jnp.full((1, depth), width), 1).astype(jnp.float32)
        table[j, 0:1] = gains[j]
        table[j, 1:2] = jnp.where(features < width, inverse, 0.0)

    square = (row_count, row_count)
    early = lax.broadcasted_iota(jnp.int32, square, 0) < lax.broadcasted_iota(jnp.int32, square, 1)
    rows = []
    for m in range(batches):
        own = ids[m]
        same = jnp.where((upright(own) == own) & early, 1, 0)
        row = jnp.sum(same, axis=0, keepdims=True) + m * capacity
        for replica, start in enumerate(starts):
            row = row + jnp.where(own == replica, start, 0)
        target[m] = row
        rows.append(row)
    row = jnp.concatenate(rows, axis=1)
    chunk_rows = slot_count * slot_rows
    source = jnp.concatenate([tokens[m] for m in range(batches)], axis=0)
    for i, chunk in enumerate(chunks):
        wanted = lax.broadcasted_iota(jnp.int32, (chunk_rows, batches * row_count), 0)
        picked = jnp.where(row == wanted + i * chunk_rows, 1.0, 0.0).astype(jnp.bfloat16)
        moved = jnp.dot(picked, source, preferred_element_type=jnp.float32).astype(jnp.bfloat16)
        for j in range(slot_count):
            chunk[j] = moved[j * slot_rows : (j + 1) * slot_rows]


def route_kernel(target, token, picked):
    for m in range(picked.shape[0]):
        wanted = upright(target[m])[:, :1]
        place = lax.broadcasted_iota(jnp.int32, picked.shape[1:], 1)
        picked[m] = jnp.where(wanted == place, 1.0, 0.0).astype(jnp.bfloat16)


def layer_kernel(has_first, has_arrived, before_count, forwards, parts, *refs):
    refs = list(refs)
    first = refs.pop(0) if has_first else None
    arrived = refs.pop(0) if has_arrived else None
    before = [refs.pop(0) for _ in range(before_count)]
    table, weight, _ = refs[:3]
    outs = refs[3:]
    if first is not None and arrived is not None:
        rows = jnp.where(lax.axis_index("section") == 0, first[0], arrived[0])
    else:
        rows = first[0] if arrived is None else arrived[0]
    rows = rows.astype(jnp.float32)
    gain, inverse = table[0, 0:1], table[0, 1:2]
    rows = jnp.where(inverse > 0.0, rows, 0.0)
    mean_square = jnp.sum(rows * rows * inverse, axis=1, keepdims=True)
    lowered = (rows * lax.rsqrt(mean_square + epsilon) * gain).astype(jnp.bfloat16)
    projected = jnp.dot(lowered, weight[0], preferred_element_type=jnp.float32)
    half = 0.5 * projected
    gate = half + half * jnp.tanh(half)
    done = (rows + jnp.where(inverse > 0.0, gate, 0.0)).astype(jnp.bfloat16)
    if forwards:
        outs.pop(0)[0] = done
    for s in range(parts):
        size = done.shape[1] // parts
        for at, ref in enumerate(before):
            outs[s][at, 0] = ref[0, :, s * size : (s + 1) * size]
        outs[s][before_count, 0] = done[:, s * size : (s + 1) * size]


def layer(first, arrived, before, token, table, weight, forwards, parts, held):
    given = [a for a in (first, arrived) if a is not None] + before
    slot_count, slot_rows, depth = given[0].shape
    block = pl.BlockSpec((1, slot_rows, depth), lambda j: (j, 0, 0))
    out_specs, out_shape = [], []
    if forwards:
        out_specs.append(block)
        out_shape.append(jax.ShapeDtypeStruct(given[0].shape, jnp.bfloat16))
    for _ in range(parts):
        size = depth // parts
        out_specs.append(pl.BlockSpec((held, 1, slot_rows, size), lambda j: (0, j, 0, 0)))
        out_shape.append(
            jax.ShapeDtypeStruct((held, slot_count, slot_rows, size), jnp.bfloat16)
        )
    return pl.pallas_call(
        functools.partial(
            layer_kernel, first is not None, arrived is not None, len(before), forwards, parts
        ),
        grid=(slot_count,),
        in_specs=[block] * len(given)
        + [
            pl.BlockSpec((1, 2, depth), lambda j: (j, 0, 0)),
            pl.BlockSpec((1, depth, depth), lambda j: (j, 0, 0)),
            ANY,
        ],
        out_specs=out_specs,
        out_shape=out_shape,
        compiler_params=pltpu.CompilerParams(vmem_limit_bytes=SMALL_VMEM),
        cost_estimate=pl.CostEstimate(
            flops=2 * slot_count * slot_rows * depth * depth,
            bytes_accessed=2 * slot_count * depth * (depth + 3 * slot_rows),
            transcendentals=0,
        ),
        name="layer",
    )(*given, table, weight, token)


def chosen(candidates):
    section = lax.axis_index("section")
    value = candidates[0]
    for s in range(1, len(candidates)):
        value = jnp.where(section == s, candidates[s], value)
    return value


def pick_kernel(sections, groups, token, *refs):
    outs = list(refs[sections * len(groups) :])
    for g, group in enumerate(groups):
        mine = refs[g * sections : (g + 1) * sections]
        for h in range(len(group)):
            out = outs.pop(0)
            for j in range(out.shape[0]):
                out[j] = chosen([ref[h, j] for ref in mine])


def combine_kernel(sections, direct, spans, picked, acc, *refs):
    out, refs = refs[-1], refs[:-1]
    rows = []
    for at in range(len(spans)):
        mine = refs[at * sections : (at + 1) * sections] if direct else refs[at : at + 1]
        for j in range(mine[0].shape[1] if direct else mine[0].shape[0]):
            rows.append(chosen([ref[0, j] for ref in mine]) if direct else mine[0][j])
    flat = jnp.concatenate(rows, axis=0)
    for m in range(out.shape[0]):
        select = jnp.concatenate([picked[m, :, low:high] for low, high in spans], axis=1)
        value = jnp.dot(select, flat, preferred_element_type=jnp.float32)
        if acc is not None:
            value = value + acc[m]
        out[m] = value.astype(out.dtype)


def schedule(rep_count):
    order = [0, 1, 4, 3, 5] + list(range(6, rep_count)) + [2]
    early = order[:-ALONE]
    sizes = SIZES if sum(SIZES) == len(early) else [-(-len(early) // 4)] * 4
    groups = [early[sum(sizes[:g]) : sum(sizes[: g + 1])] for g in range(len(sizes))]
    return order, groups, order[-ALONE:]


def on_device(tokens, replica_of_row, widths, placement, gains, weights):
    batches, row_count, depth = tokens.shape
    rep_count = lax.axis_size("rep")
    section_count = lax.axis_size("section")
    slot_count = weights.shape[1]
    replica_count = widths.shape[0]
    capacity = (3 * row_count + 2 * replica_count - 1) // (2 * replica_count)
    last = section_count - 1
    part = depth // section_count
    slot_rows = batches * capacity
    chunk_rows = slot_count * slot_rows

    gain = gains.reshape(slot_count, 1, depth)
    weight = weights.reshape(slot_count, depth, depth)
    ids = replica_of_row.reshape(batches, 1, row_count)
    chunk_shape = jax.ShapeDtypeStruct((slot_count, slot_rows, depth), jnp.bfloat16)
    opened = pl.pallas_call(
        open_kernel,
        in_specs=[],
        out_specs=VMEM,
        out_shape=jax.ShapeDtypeStruct((8, 128), jnp.float32),
        compiler_params=pltpu.CompilerParams(vmem_limit_bytes=1024 * 1024),
        cost_estimate=pl.CostEstimate(
            flops=16 * 1024**3, bytes_accessed=64 * 1024**2, transcendentals=0
        ),
        name="open",
    )()
    target, table, *outgoing = pl.pallas_call(
        functools.partial(
            dispatch_kernel, (batches, row_count, slot_count, capacity, depth)
        ),
        in_specs=[SMEM, SMEM, VMEM, VMEM, VMEM, ANY],
        out_specs=[VMEM] * (rep_count + 2),
        out_shape=[
            jax.ShapeDtypeStruct(ids.shape, jnp.int32),
            jax.ShapeDtypeStruct((slot_count, 2, depth), jnp.float32),
        ]
        + [chunk_shape] * rep_count,
        compiler_params=pltpu.CompilerParams(vmem_limit_bytes=VMEM_LIMIT),
        cost_estimate=pl.CostEstimate(
            flops=2 * batches * row_count * rep_count * chunk_rows * depth,
            bytes_accessed=2 * depth * (batches * row_count + rep_count * chunk_rows),
            transcendentals=0,
        ),
        name="dispatch",
    )(placement, widths, ids, tokens, gain, opened)

    def traded(x, i):
        if i == 0:
            return x
        return lax.ppermute(x, "rep", [(d, d ^ i) for d in range(rep_count)])

    order, groups, direct = schedule(rep_count)

    def arriving(x, i):
        if i == 0:
            return x
        hops = [
            (s * rep_count + d, s * rep_count + (d ^ (i if s == 0 else 1)))
            for s in range(section_count)
            for d in range(rep_count)
        ]
        return lax.ppermute(x, ("section", "rep"), hops)

    entering = {i: arriving(outgoing[i], i) for i in order}

    def sent_back(pieces, hop):
        sent = []
        for s, piece in enumerate(pieces):
            if s != last or hop != 0:
                hops = [(last * rep_count + d, s * rep_count + (d ^ hop)) for d in range(rep_count)]
                if s == last:
                    hops += [
                        (t * rep_count + d, t * rep_count + (d ^ 1))
                        for t in range(last)
                        for d in range(rep_count)
                    ]
                piece = lax.ppermute(piece, ("section", "rep"), hops)
            sent.append(piece)
        return sent

    lag = STREAMS * last
    inbound, finished, back = {}, {}, {}
    token = target
    picked = None
    for n in range(rep_count + lag):
        first = entering[order[n]] if n < rep_count else None
        arrived = inbound.get(n)
        closing = groups + [[i] for i in direct]
        group = next((g for g in closing if n >= lag and g[-1] == order[n - lag]), None)
        before = [finished[i] for i in group[:-1]] if group else []
        opens = n >= lag and group is None
        forward = [(s, s + 1) for s in range(last) if 0 <= n - STREAMS * s < rep_count]
        forwards = n < rep_count + lag - STREAMS or opens
        made = layer(
            first,
            arrived,
            before,
            token,
            table,
            weight,
            forwards,
            section_count if group else 0,
            len(group) if group else 0,
        )
        token = made[0]
        if n < rep_count + lag - STREAMS:
            inbound[n + STREAMS] = lax.ppermute(made[0], "section", forward)
        if opens:
            finished[order[n - lag]] = made[0]
        if group:
            hop = group[0] if group[0] in direct else 0
            back[group[0]] = sent_back(made[-section_count:], hop)
        if n == 1:
            token = picked = pl.pallas_call(
                route_kernel,
                in_specs=[VMEM, ANY],
                out_specs=VMEM,
                out_shape=jax.ShapeDtypeStruct(
                    (batches, row_count, rep_count * chunk_rows), jnp.bfloat16
                ),
                compiler_params=pltpu.CompilerParams(vmem_limit_bytes=SMALL_VMEM),
                name="route",
            )(target, token)

    mine = pl.pallas_call(
        functools.partial(pick_kernel, section_count, groups),
        in_specs=[ANY] + [VMEM] * (section_count * len(groups)),
        out_specs=[VMEM] * (rep_count - len(direct)),
        out_shape=[jax.ShapeDtypeStruct((slot_count, slot_rows, part), jnp.bfloat16)]
        * (rep_count - len(direct)),
        compiler_params=pltpu.CompilerParams(vmem_limit_bytes=SMALL_VMEM),
        name="pick",
    )(token, *[piece for group in groups for piece in back[group[0]]])
    early = order[: len(mine)]
    returned = []
    for i, piece in zip(early, mine):
        returned.append(traded(piece, i))

    def combined(these, acc, given, dtype, is_direct):
        spans = [(i * chunk_rows, (i + 1) * chunk_rows) for i in these]

        def kernel(picked, *refs):
            refs = list(refs)
            some = refs.pop(0) if acc is not None else None
            combine_kernel(section_count, is_direct, spans, picked, some, *refs)

        extra = [] if acc is None else [acc]
        return pl.pallas_call(
            kernel,
            in_specs=[VMEM] * (1 + len(extra) + len(given)),
            out_specs=VMEM,
            out_shape=jax.ShapeDtypeStruct((batches, row_count, part), dtype),
            compiler_params=pltpu.CompilerParams(vmem_limit_bytes=SMALL_VMEM),
            name="combine",
        )(picked, *extra, *given)

    acc = combined(early, None, returned, jnp.float32, False)
    late = [piece for i in direct for piece in back[i]]
    return combined(direct, acc, late, jnp.bfloat16, True)


def solution(mesh):
    placed = (
        P(None, "rep", None),
        P(None, "rep", None),
        P(),
        P(),
        P("section", "rep", None),
        P("section", "rep", None, None),
    )

    return jax.shard_map(
        on_device, mesh=mesh, in_specs=placed, out_specs=P(None, "rep", "section"), check_vma=False
    )
```
